512 devices in a mesh: space: 128 (over z, y, core), ens: 4 (over x).
Axes of the slice: x: 4, y: 8, z: 8, core: 2. Of those that a mesh axis runs over, the one named last changes fastest.
Arguments:
- innovations: bfloat16 [4, 8192, 128, 128], P('ens', 'space'), may hold values from -6 to 6
- block_owner: int32 [8192, 1], P('space'), may hold values from 0 to 127; in each aligned block of 64 rows (0 to 63, 64 to 127, ...) at most 2 rows name the same one
- block_tile: int32 [8192], P('space'), may hold values from 0 to 3
- block_count: int32 [128], P('space'), may hold values from 48 to 64
- obs_row: int32 [8192, 128], P('space'), may hold values from 0 to 6
- obs_col: int32 [8192, 128], P('space'), may hold values from 0 to 14
- offsets: float32 [8192, 2, 128], P('space'), may hold values from 0 to 1
- obs_mask: int32 [8192, 128], P('space'), may hold values 0 or 1
- sigma: float32 [512, 128], P('space'), may hold values from 0.3 to 3
- coupling: float32 [128, 128], replicated, may hold values from -0.5 to 0.5
Outputs:
- gradient: float32 [128, 512, 128], P('ens', 'space')
The draws below stay inside these ranges and needn't reach their ends.
Inputs may be any that keep to these rules, and one draw needn't show every extreme that they name: `block_owner`: among the rows of one device, no owner is named more than 2 times, and one owner is named exactly 2 times in some devices' rows. `block_count`: blocks of a device at positions at or above its count are padding.
All inputs are finite; a program needn't handle non-finite values. No bound on the sum of `obs_mask` on one device may be relied on, other than what follows from the above.
Results may differ from the reference program's by a relative error of at most 0.0095.
Values may be sent and summed in bfloat16 or wider, within the bound.
A program may use at most 64 MiB of HBM per device.

```python
import math
import jax
import jax.numpy as jnp
import numpy as np
from jax import lax

CH = 128
OBS = 128
TH = 8
TW = 16
CELLS = 128
TILE_DEV = 4
TILES = 512
BLK_DEV = 64
BLOCKS = 8192
CAP = 2
MEMBERS = 4
N_SPACE = 128


def with_ends(array, own_key, low, largest):
    place = [jax.random.randint(jax.random.fold_in(own_key, axis), (), 0, length) for axis, length in enumerate(array.shape)]
    main_axis = array.shape.index(max(array.shape))
    beside = place[:main_axis] + [(place[main_axis] + 1) % array.shape[main_axis]] + place[main_axis + 1:]
    return array.at[tuple(place)].set(low).at[tuple(beside)].set(largest)


def levels(own_key, shape, pieces, least, high):
    def one(dim, blocks):
        draws = jax.random.uniform(jax.random.fold_in(jax.random.fold_in(own_key, 6), dim), (blocks,), jnp.float32, least / len(pieces), high / len(pieces))
        return jnp.repeat(jnp.exp(draws), shape[dim] // blocks).reshape((-1,) + (1,) * (len(shape) - dim - 1))

    loudness = one(*pieces[0])
    for cut in pieces[1:]:
        loudness = loudness * one(*cut)
    return loudness


def routed_block(stream_key, own, number, rows, amount, top, reach, skew):
    order = jax.random.permutation(stream_key, amount)
    crowded, common = shares(amount, rows * top, reach, skew, True), shares(amount, rows * top, reach, skew, False)
    places = jnp.arange(amount)

    def named(sizes, rotation):
        used = int((sizes > 0).sum())
        fixed = max(1, used // 4)
        shifted = fixed + (places - fixed + rotation * (used - fixed)) % max(1, amount - fixed)
        return jnp.zeros((amount,), jnp.int32).at[order[jnp.where(places < fixed, places, shifted)]].set(jnp.asarray(sizes, jnp.int32))

    sizes = jnp.where(number % 4 == 0, named(crowded, number // 4), named(common, number - number // 4 - 1))
    mixed = jax.random.permutation(jax.random.fold_in(own, 3), amount)
    donor, taker = mixed[0:amount // 2 * 2:2], mixed[1:amount // 2 * 2:2]
    margin = jnp.minimum(sizes[donor] - 1, reach - sizes[taker]) // 2
    margin = jnp.where((donor == order[0]) | (taker == order[0]) | (sizes[taker] == 0), 0, jnp.maximum(margin, 0))
    shifted = jax.random.randint(jax.random.fold_in(own, 4), (amount // 2,), 0, 1 << 20) % (margin + 1)
    sizes = sizes.at[donor].add(-shifted).at[taker].add(shifted)
    labels = jnp.searchsorted(jnp.cumsum(sizes), jnp.arange(rows * top), side="right").astype(jnp.int32)
    grid = labels.reshape(top, rows).T
    grid = grid[jax.random.permutation(jax.random.fold_in(own, 1), rows)]
    rotation = jax.random.randint(jax.random.fold_in(own, 2), (rows, 1), 0, top)
    return jnp.take_along_axis(grid, (jnp.arange(top)[None, :] + rotation) % top, axis=1)


def shares(amount, total, bound, lean, full):
    loads = [(1 << 20) // math.isqrt(rank ** lean) + 1 for rank in range(1, amount + 1)]
    largest = bound if full else min(bound, max(-(-total // amount), total * loads[0] // sum(loads)))
    least = 1 if total - largest >= amount - 1 else 0
    holding, rest = [largest] + [least] * (amount - 1), total - largest - least * (amount - 1)
    while rest > 0:
        free = [i for i in range(1, amount) if holding[i] < largest] or [i for i in range(1, amount) if holding[i] < bound]
        pool, remaining = sum([loads[i] for i in free]), rest
        for i in free:
            extra = min(bound - holding[i], max(1, remaining * loads[i] // pool), rest)
            holding[i] = holding[i] + extra
            rest = rest - extra
    return np.array(holding)


def noise(own_key, extent, width, bound, cuts=(), kind=jnp.bfloat16):
    array = jax.random.normal(own_key, extent, jnp.float32) * width
    if len(cuts) > 0:
        array = levels(own_key, extent, cuts, -0.22, 0.18) * array
    return jnp.clip(array, min=-bound, max=bound).astype(kind)


def setup_inputs(seed: int = 0) -> dict:
    keys = jax.random.split(jax.random.key(seed), 11)
    innovations = noise(keys[0], (MEMBERS, BLOCKS, OBS, CH), 1.0, 6.0, ((0, 4), (1, 128)))
    block_owner_keys = jax.random.split(jax.random.fold_in(keys[1], 1), BLOCKS // BLK_DEV)
    block_owner_turns = jax.random.permutation(jax.random.fold_in(keys[1], 3), BLOCKS // BLK_DEV)
    block_owner = jax.vmap(lambda own, number: routed_block(jax.random.fold_in(keys[1], 2), own, number, BLK_DEV, N_SPACE, 1, CAP, 2))(block_owner_keys, block_owner_turns).reshape((BLOCKS, 1))
    block_tile = with_ends(jax.random.randint(keys[2], (BLOCKS,), 0, TILE_DEV), jax.random.fold_in(keys[2], 1), 0, TILE_DEV - 1).astype(jnp.int32)
    block_count = with_ends(jax.random.randint(keys[3], (N_SPACE,), 3 * BLK_DEV // 4, BLK_DEV + 1), jax.random.fold_in(keys[3], 1), 3 * BLK_DEV // 4, BLK_DEV).astype(jnp.int32)
    obs_row = with_ends(jax.random.randint(keys[4], (BLOCKS, OBS), 0, TH - 1), jax.random.fold_in(keys[4], 1), 0, (TH - 1) - 1).astype(jnp.int32)
    obs_col = with_ends(jax.random.randint(keys[5], (BLOCKS, OBS), 0, TW - 1), jax.random.fold_in(keys[5], 1), 0, (TW - 1) - 1).astype(jnp.int32)
    offsets = jnp.clip(1.0 * jax.random.uniform(keys[6], (BLOCKS, 2, OBS), jnp.float32) ** levels(keys[6], (BLOCKS, 2, OBS), ((0, 128),), -0.2, 0.2), 0.0, 1.0)
    obs_mask = with_ends((jax.random.randint(keys[7], (BLOCKS, OBS), 0, 4) < 3).astype(jnp.int32), jax.random.fold_in(keys[7], 1), 0, 1)
    sigma = jnp.clip(jnp.exp(math.log(3.0) - 2.3025851 * jax.random.uniform(keys[8], (TILES, CH), jnp.float32) ** levels(keys[8], (TILES, CH), ((0, 128),), -0.2, 0.2)), 0.3, 3.0)
    coupling = noise(keys[9], (CELLS, CELLS), CELLS ** -0.5, 0.5, (), jnp.float32)
    return {"innovations": innovations, "block_owner": block_owner, "block_tile": block_tile, "block_count": block_count, "obs_row": obs_row, "obs_col": obs_col, "offsets": offsets, "obs_mask": obs_mask, "sigma": sigma, "coupling": coupling}


def reference(innovations, block_owner, block_tile, block_count, obs_row, obs_col, offsets, obs_mask, sigma, coupling):
    blocks = block_owner.shape[0]
    per_device = blocks // block_count.shape[0]
    position = jnp.arange(blocks, dtype=jnp.int32)
    alive = (position % per_device) < block_count[position // per_device]
    live = obs_mask.astype(jnp.float32) * alive[:, None].astype(jnp.float32)
    row_frac = offsets[:, 0, :]
    col_frac = offsets[:, 1, :]
    tile = block_owner[:, 0] * TILE_DEV + block_tile
    summed = jnp.sum(innovations.astype(jnp.float32), axis=0).reshape(-1, CH)
    total = jnp.zeros((TILES * CELLS, CH), jnp.float32)
    for down in (0, 1):
        for right in (0, 1):
            row_part = row_frac if down == 1 else 1.0 - row_frac
            col_part = col_frac if right == 1 else 1.0 - col_frac
            rounded = (row_part * col_part * live).astype(jnp.bfloat16)
            rounded = lax.optimization_barrier(rounded).astype(jnp.float32)
            target = tile[:, None] * CELLS + (obs_row + down) * TW + obs_col + right
            total = total.at[target.reshape(-1)].add(summed * rounded.reshape(-1, 1))
    mean = total.reshape(TILES, CELLS, CH) / MEMBERS
    coupled = jnp.einsum("ck,tkh->cth", coupling, mean, precision=lax.Precision.HIGHEST)
    return sigma[None, :, :] * (jnp.transpose(mean, (1, 0, 2)) + coupled)
```

```python
import jax
import jax.numpy as jnp
from jax import lax
from jax.experimental import pallas as pl
from jax.experimental.pallas import tpu as pltpu
from jax.sharding import PartitionSpec as P

MESH = pl.DeviceIdType.MESH
F32 = jnp.float32
BF16 = jnp.bfloat16
NX = 4
NR = 8
ROWS = 8
TW = 16
BLK = 64
CHUNK = 8
FAR = ((4, 3), (6, 1), (5, 2), (7, 0))


def kernel(
    key_ref,
    count_ref,
    inn_hbm,
    row_ref,
    col_ref,
    off_ref,
    mask_ref,
    sigma_ref,
    coup_ref,
    out_ref,
    inn,
    csend,
    fwd,
    comb,
    recv,
    other,
    vals,
    asend,
    arecv,
    fin,
    brecv,
    mean,
    gath,
    maps,
    mapo,
    smap,
    in_sem,
    fsend_sem,
    frecv_sem,
    nsend_sem,
    nrecv_sem,
    dsend_sem,
    drecv_sem,
    msend_sem,
    mrecv_sem,
    local_sem,
    asend_sem,
    arecv_sem,
    bsend_sem,
    brecv_sem,
    gsend_sem,
    grecv_sem,
):
    s = lax.axis_index("space")
    x = lax.axis_index("ens")
    c = lax.rem(s, 2)
    y = lax.rem(lax.div(s, 2), NR)
    z = lax.div(s, 2 * NR)
    chip = s - c
    a = y + c * (z - y)
    b = z + c * (y - z)
    stride_a = 2 + (2 * NR - 2) * c
    stride_b = 2 * NR - (2 * NR - 2) * c
    me = 2 * x + c

    def wrap(value, size):
        return lax.rem(value + 2 * size, size)

    def group_device(dx, dc):
        return {"space": chip + wrap(c + dc, 2), "ens": wrap(x + dx, NX)}

    def ring_device(da, db):
        return {"space": wrap(a + da, NR) * stride_a + wrap(b + db, NR) * stride_b + c, "ens": x}

    def load(ch):
        blocks = pl.ds(ch * CHUNK, CHUNK)
        return pltpu.make_async_copy(inn_hbm.at[blocks], inn.at[blocks], in_sem.at[ch])

    for j in range(8):
        load((j >> 1) + 4 * (j & 1)).start()

    barrier = pltpu.get_barrier_semaphore()
    partners = [group_device(dx, dc) for dx in range(NX) for dc in range(2) if (dx, dc) != (0, 0)]
    partners += [ring_device(1, 0), ring_device(-1, 0)]
    partners += [ring_device(0, r) for r in range(1, NR)]
    for partner in partners:
        pl.semaphore_signal(barrier, inc=1, device_id=partner, device_id_type=MESH)

    sub = lax.broadcasted_iota(jnp.int32, (8, 128), 0)
    lane = lax.broadcasted_iota(jnp.int32, (8, 128), 1)
    tile_ids = lax.rem(sub, 4) * 128 + lane

    def note(i, found):
        first, last = found
        hit = tile_ids == key_ref[i]
        return jnp.minimum(first, jnp.where(hit, i, BLK)), jnp.maximum(last, jnp.where(hit, i, -1))

    first, last = lax.fori_loop(
        0, BLK, note, (jnp.full((8, 128), BLK, jnp.int32), jnp.full((8, 128), -1, jnp.int32))
    )
    second = jnp.where((last == first) | (last < 0), BLK, last)
    maps[...] = jnp.where(sub < 4, first, second)
    for rel in range(2):
        vals[rel, BLK] = jnp.zeros((TW, 128), F32)

    def far_copy(par, i):
        sign = 1 - 2 * par
        blocks = pl.ds((4 * par + i) * CHUNK, CHUNK)
        return pltpu.make_async_remote_copy(
            src_ref=csend.at[pl.ds(2 * wrap(x + 2, NX), 2), blocks],
            dst_ref=fwd.at[par, i],
            send_sem=fsend_sem.at[par, i],
            recv_sem=frecv_sem.at[par, i],
            device_id={"space": s, "ens": wrap(x + sign, NX)},
            device_id_type=MESH,
        )

    def near_copy(slot, ch, rel, src):
        sign = 1 - 2 * slot
        return pltpu.make_async_remote_copy(
            src_ref=src,
            dst_ref=recv.at[slot, rel, pl.ds(ch * CHUNK, CHUNK)],
            send_sem=nsend_sem.at[slot, rel, ch],
            recv_sem=nrecv_sem.at[slot, rel, ch],
            device_id={"space": chip + wrap(c + rel, 2), "ens": wrap(x + sign, NX)},
            device_id_type=MESH,
        )

    def near_own(slot, ch, rel):
        sign = 1 - 2 * slot
        row = 2 * wrap(x + sign, NX) + wrap(c + rel, 2)
        return near_copy(slot, ch, rel, csend.at[row, pl.ds(ch * CHUNK, CHUNK)])

    def near_comb(par, i, rel):
        return near_copy(par, 4 * par + i, rel, comb.at[par, i, rel])

    def core_copy(ch):
        blocks = pl.ds(ch * CHUNK, CHUNK)
        return pltpu.make_async_remote_copy(
            src_ref=csend.at[2 * x + 1 - c, blocks],
            dst_ref=other.at[blocks],
            send_sem=dsend_sem.at[ch],
            recv_sem=drecv_sem.at[ch],
            device_id=group_device(0, 1),
            device_id_type=MESH,
        )

    def map_copy():
        return pltpu.make_async_remote_copy(
            src_ref=maps,
            dst_ref=mapo,
            send_sem=msend_sem,
            recv_sem=mrecv_sem,
            device_id=group_device(0, 1),
            device_id_type=MESH,
        )

    iota8 = lax.broadcasted_iota(jnp.int32, (ROWS, 128), 0)
    iota16 = lax.broadcasted_iota(jnp.int32, (TW, 128), 0)
    count = count_ref[0]

    def first_phase(j, carry):
        par = lax.rem(j, 2)
        i = lax.div(j, 2)
        ch = 4 * par + i
        start = pl.multiple_of(ch * CHUNK, CHUNK)
        load(ch).wait()
        rows = row_ref[pl.ds(start, CHUNK), :]
        cols = col_ref[pl.ds(start, CHUNK), :]
        masks = mask_ref[pl.ds(start, CHUNK), :]
        for k in range(CHUNK):
            block = start + k
            fracs = off_ref[block]
            fy, fx = fracs[0:1], fracs[1:2]
            alive = jnp.where(block < count, 1.0, 0.0).astype(F32)
            live = masks[k : k + 1].astype(F32) * alive
            down = iota8 - rows[k : k + 1]
            right = iota16 - cols[k : k + 1]
            row_part = jnp.where(down == 0, 1.0 - fy, jnp.where(down == 1, fy, 0.0)) * live
            col_part = jnp.where(right == 0, 1.0 - fx, jnp.where(right == 1, fx, 0.0))
            table = (row_part[:, None, :] * col_part[None, :, :]).astype(BF16)
            table = table.reshape(ROWS * TW, 128)
            done = jnp.dot(table, inn[block], preferred_element_type=F32).astype(BF16)
            for g in range(ROWS):
                csend[g, block] = done[g * TW : (g + 1) * TW]

        @pl.when(j == 0)
        def _():
            pl.semaphore_wait(barrier, len(partners))
            map_copy().start()

        far_copy(par, i).start()
        near_own(1 - par, ch, 0).start()
        near_own(1 - par, ch, 1).start()
        core_copy(ch).start()
        return carry

    lax.fori_loop(0, 8, first_phase, 0)

    def merge(j, carry):
        par = lax.rem(j, 2)
        i = lax.div(j, 2)
        sign = 1 - 2 * par
        far_copy(par, i).wait_recv()
        for rel in range(2):
            core = wrap(c + rel, 2)
            row = 2 * wrap(x + sign, NX) + core

            def add(k, inner):
                block = (4 * par + i) * CHUNK + k
                comb[par, i, rel, k] = (
                    fwd[par, i, core, k].astype(F32) + csend[row, block].astype(F32)
                ).astype(BF16)
                return inner

            lax.fori_loop(0, CHUNK, add, 0, unroll=True)
            near_comb(par, i, rel).start()
        return carry

    lax.fori_loop(0, 8, merge, 0)

    own_map = pltpu.make_async_copy(maps, smap.at[0], local_sem.at[0])
    own_map.start()
    map_copy().wait_recv()
    other_map = pltpu.make_async_copy(mapo, smap.at[1], local_sem.at[1])
    other_map.start()
    own_map.wait()
    other_map.wait()

    def sum_members(j, carry):
        ch = 4 * lax.rem(j, 2) + lax.div(j, 2)
        core_copy(ch).wait_recv()
        for slot in range(2):
            for rel in range(2):
                near_own(slot, ch, rel).wait_recv()

        def add(k, inner):
            block = ch * CHUNK + k
            vals[0, block] = (
                recv[0, 0, block].astype(F32)
                + recv[1, 0, block].astype(F32)
                + csend[me, block].astype(F32)
            )
            vals[1, block] = (
                recv[0, 1, block].astype(F32)
                + recv[1, 1, block].astype(F32)
                + other[block].astype(F32)
            )
            return inner

        lax.fori_loop(0, CHUNK, add, 0, unroll=True)
        return carry

    lax.fori_loop(0, 8, sum_members, 0)

    def own_sum(t):
        hi, lo = lax.div(t, 128), lax.rem(t, 128)
        return (
            vals[0, smap[0, hi, lo]]
            + vals[0, smap[0, 4 + hi, lo]]
            + vals[1, smap[1, hi, lo]]
            + vals[1, smap[1, 4 + hi, lo]]
        )

    def ring_copy(way, step, q):
        return pltpu.make_async_remote_copy(
            src_ref=asend.at[way, step, q],
            dst_ref=arecv.at[way, step, q],
            send_sem=asend_sem.at[way, step, q],
            recv_sem=arecv_sem.at[way, step, q],
            device_id=ring_device(1 - 2 * way, 0),
            device_id_type=MESH,
        )

    steps = NR // 2
    for step in range(steps):
        for place in range(4):
            if step == 0 and place < 2:
                continue
            for way in range(2):
                q = (place + 2 * (1 - way)) % 4
                got = step > 1 or (step == 1 and place >= 2)
                if got:
                    ring_copy(way, step - 1, q).wait_recv()
                to_a = wrap(a + (1 - 2 * way) * (steps - step), NR)
                for half in range(2):
                    to_b = wrap(b + FAR[q][half], NR)
                    base = 4 * (to_a * stride_a + to_b * stride_b)

                    def add(k, inner):
                        total = own_sum(base + k)
                        if got:
                            total = total + arecv[way, step - 1, q, half * 8 + k].astype(F32)
                        asend[way, step, q, half * 8 + k] = total.astype(BF16)
                        return inner

                    lax.fori_loop(0, 8, add, 0, unroll=True)
                ring_copy(way, step, q).start()

    def line_copy(r):
        return pltpu.make_async_remote_copy(
            src_ref=fin.at[r],
            dst_ref=brecv.at[r],
            send_sem=bsend_sem.at[r],
            recv_sem=brecv_sem.at[r],
            device_id=ring_device(0, r),
            device_id_type=MESH,
        )

    for q in (0, 2, 1, 3):
        ring_copy(0, steps - 1, q).wait_recv()
        ring_copy(1, steps - 1, q).wait_recv()
        for half in range(2):
            r = FAR[q][half]
            base = 4 * (a * stride_a + wrap(b + r, NR) * stride_b)

            def add(k, inner):
                total = own_sum(base + k)
                for way in range(2):
                    total = total + arecv[way, steps - 1, q, half * 8 + k].astype(F32)
                if r == 0:
                    mean[k] = total
                else:
                    fin[r, k] = total.astype(BF16)
                return inner

            lax.fori_loop(0, 8, add, 0, unroll=True)
            if r != 0:
                line_copy(r).start()

    for r in range(1, NR):
        line_copy(r).wait_recv()

    def finish(k, carry):
        total = mean[k]
        for r in range(1, NR):
            total = total + brecv[r, k].astype(F32)
        fin[0, k] = total.astype(BF16)
        return carry

    lax.fori_loop(0, 8, finish, 0, unroll=True)

    def gather_copy(dx, dc):
        core = wrap(c + dc, 2)
        return pltpu.make_async_remote_copy(
            src_ref=fin.at[0, pl.ds(4 * core, 4)],
            dst_ref=gath.at[me],
            send_sem=gsend_sem.at[2 * dx + dc],
            recv_sem=grecv_sem.at[2 * dx + dc],
            device_id=group_device(dx, dc),
            device_id_type=MESH,
        )

    others = [(2, 0), (2, 1), (1, 0), (1, 1), (3, 0), (3, 1), (0, 1)]
    for dx, dc in others:
        gather_copy(dx, dc).start()
    for t in range(4):
        gath[me, t] = fin[0, 4 * c + t]

    def sent(j, carry):
        par = lax.rem(j, 2)
        i = lax.div(j, 2)
        far_copy(par, i).wait_send()
        core_copy(j).wait_send()
        for rel in range(2):
            near_own(0, j, rel).wait_send()
            near_own(1, j, rel).wait_send()
        return carry

    lax.fori_loop(0, 8, sent, 0)
    map_copy().wait_send()
    for step in range(steps):
        for place in range(4):
            if step == 0 and place < 2:
                continue
            for way in range(2):
                ring_copy(way, step, (place + 2 * (1 - way)) % 4).wait_send()
    for r in range(1, NR):
        line_copy(r).wait_send()

    coup = coup_ref[pl.ds(pl.multiple_of(32 * x, 32), 32), :]
    coup_hi = coup.astype(BF16)
    coup_lo = (coup - coup_hi.astype(F32)).astype(BF16)
    for dx, dc in others:
        gather_copy(dx, dc).wait_recv()
    for t in range(4):
        field = jnp.concatenate([gath[g, t] for g in range(ROWS)], axis=0)
        own = jnp.concatenate([gath[2 * x, t], gath[2 * x + 1, t]], axis=0).astype(F32)
        coupled = jnp.dot(coup_hi, field, preferred_element_type=F32)
        coupled = coupled + jnp.dot(coup_lo, field, preferred_element_type=F32)
        scaled = (own + coupled) * (sigma_ref[t : t + 1, :] * (1.0 / NX))
        out_ref[:, t, :] = scaled
    for dx, dc in others:
        gather_copy(dx, dc).wait_send()


def on_device(
    innovations,
    block_owner,
    block_tile,
    block_count,
    obs_row,
    obs_col,
    offsets,
    obs_mask,
    sigma,
    coupling,
):
    key = block_owner[:, 0] * 4 + block_tile
    vmem = pl.BlockSpec(memory_space=pltpu.VMEM)
    smem = pl.BlockSpec(memory_space=pltpu.SMEM)
    dma = pltpu.SemaphoreType.DMA
    tile = (TW, 128)
    return pl.pallas_call(
        kernel,
        out_shape=jax.ShapeDtypeStruct((32, 4, 128), F32),
        in_specs=[smem, smem, pl.BlockSpec(memory_space=pltpu.HBM)] + [vmem] * 6,
        out_specs=vmem,
        scratch_shapes=[
            pltpu.VMEM((BLK, 128, 128), BF16),
            pltpu.VMEM((ROWS, BLK) + tile, BF16),
            pltpu.VMEM((2, 4, 2, CHUNK) + tile, BF16),
            pltpu.VMEM((2, 4, 2, CHUNK) + tile, BF16),
            pltpu.VMEM((2, 2, BLK) + tile, BF16),
            pltpu.VMEM((BLK,) + tile, BF16),
            pltpu.VMEM((2, BLK + 1) + tile, F32),
            pltpu.VMEM((2, 4, 4, 16) + tile, BF16),
            pltpu.VMEM((2, 4, 4, 16) + tile, BF16),
            pltpu.VMEM((NR, 8) + tile, BF16),
            pltpu.VMEM((NR, 8) + tile, BF16),
            pltpu.VMEM((8,) + tile, F32),
            pltpu.VMEM((ROWS, 4) + tile, BF16),
            pltpu.VMEM((8, 128), jnp.int32),
            pltpu.VMEM((8, 128), jnp.int32),
            pltpu.SMEM((2, 8, 128), jnp.int32),
            dma((8,)),
            dma((2, 4)),
            dma((2, 4)),
            dma((2, 2, 8)),
            dma((2, 2, 8)),
            dma((8,)),
            dma((8,)),
            dma,
            dma,
            dma((2,)),
            dma((2, 4, 4)),
            dma((2, 4, 4)),
            dma((NR,)),
            dma((NR,)),
            dma((8,)),
            dma((8,)),
        ],
        compiler_params=pltpu.CompilerParams(
            collective_id=0, has_side_effects=True, vmem_limit_bytes=48 * 1024 * 1024
        ),
        name="adjoint",
    )(
        key,
        block_count,
        innovations[0],
        obs_row,
        obs_col,
        offsets,
        obs_mask,
        sigma,
        coupling,
    )


def solution(mesh):
    in_specs = (
        P("ens", "space", None, None),
        P("space", None),
        P("space"),
        P("space"),
        P("space", None),
        P("space", None),
        P("space", None, None),
        P("space", None),
        P("space", None),
        P(),
    )
    return jax.shard_map(
        on_device,
        mesh=mesh,
        in_specs=in_specs,
        out_specs=P("ens", "space", None),
        check_vma=False,
    )
```
